32 devices in a mesh: dp: 32 (over z, y, x, core).
Axes of the slice: x: 2, y: 2, z: 4, core: 2. Of those that a mesh axis runs over, the one named last changes fastest.
Arguments:
- grads: float32 [32, 163840], P('dp'), may hold values from -6 to 6
- master: float32 [163840], P('dp')
- moment1: float32 [163840], P('dp'), may hold values from -4 to 4
- moment2: float32 [163840], P('dp'), may hold values from 0.1 to 2
- tensor_rows: int32 [8], replicated, may hold values from 1 to 16, 32 in all
- step_count: int32 [1], replicated, may hold values from 1 to 19
Outputs:
- new_weights: bfloat16 [163840], replicated
- new_master: float32 [163840], P('dp')
- new_moment1: float32 [163840], P('dp')
- new_moment2: float32 [163840], P('dp')
The draws below stay inside these ranges and needn't reach their ends.
All inputs are finite; a program needn't handle non-finite values.
Results may differ from the reference program's by a relative error of at most 0.001.
Values may be sent and summed in bfloat16 or wider, within the bound.
A program may use at most 64 MiB of HBM per device.

```python
import math
import jax
import jax.numpy as jnp
import numpy as np
from jax import lax

D = 5120
NSEG = 8
ROWS = 32
P_SIZE = 163840
N_DP = 32


def draw_master(key, part):
    base_key, row_key, col_key = jax.random.split(jax.random.fold_in(key, 17), 3)
    base = jax.random.normal(base_key, (ROWS, D), jnp.float32)
    position = jnp.arange(ROWS, dtype=jnp.float32) / jnp.float32(ROWS)
    row_scale = jnp.exp(jax.random.uniform(row_key, (ROWS, 1), jnp.float32, 0.0, math.log(10.0)))
    row_scale = row_scale * jnp.power(3.0, position)[:, None]
    col_scale = jnp.exp(jax.random.uniform(col_key, (1, D), jnp.float32, 0.0, math.log(4.0)))
    return (0.1 * base * row_scale * col_scale).reshape(P_SIZE).astype(jnp.float32)


def strengthened(entries, rng, source, target, shards_of, factor):
    def block_of(dim):
        return (jnp.arange(entries.shape[dim]) // (entries.shape[dim] // shards_of)).reshape((-1,) + (1,) * (entries.ndim - 1 - dim))

    first = jax.random.permutation(rng, shards_of)[block_of(target)]
    far = (block_of(target) + shards_of // 2) % shards_of
    return jnp.where((block_of(source) == first) | (block_of(source) == far), factor * entries, entries)


def shard_levels(own_key, extent, pieces, least, largest):
    def one(dim, parts):
        heights = jax.random.uniform(jax.random.fold_in(jax.random.fold_in(own_key, 6), dim), (parts,), jnp.float32, least / len(pieces), largest / len(pieces))
        return jnp.repeat(jnp.exp(heights), extent[dim] // parts).reshape((-1,) + (1,) * (len(extent) - dim - 1))

    factor_of = one(*pieces[0])
    for cut in pieces[1:]:
        factor_of = factor_of * one(*cut)
    return factor_of


def split_up(number_of, total, bound, lean):
    weights = [(1 << 20) // math.isqrt(rank ** lean) + 1 for rank in range(2, number_of + 1)]
    surplus, given = total - bound - (number_of - 1), [1] * (number_of - 1)
    while surplus > 0:
        candidates = [i for i in range(number_of - 1) if given[i] < bound]
        pool, remaining = sum([weights[i] for i in candidates]), surplus
        for i in candidates:
            addition = min(bound - given[i], max(1, remaining * weights[i] // pool), surplus)
            given[i] = given[i] + addition
            surplus = surplus - addition
    return np.array([bound] + given)


def uneven_parts(rng, count, total, most, skew):
    if count == 2:
        one = jax.random.randint(rng, (), max(1, total - most), min(most, total - 1) + 1)
        return jnp.stack([one, total - one])
    sizes = jnp.asarray(split_up(count, total, most, skew), jnp.int32)
    pairs = (count - 1) // 2
    giver, taker = sizes[1:1 + 2 * pairs:2], sizes[2:2 + 2 * pairs:2]
    margin = jnp.minimum(giver - 1, most - taker)
    passed = jax.random.randint(jax.random.fold_in(rng, 1), (pairs,), 0, 1 << 20) % (margin + 1)
    sizes = sizes.at[1:1 + 2 * pairs:2].set(giver - passed).at[2:2 + 2 * pairs:2].set(taker + passed)
    return sizes[jax.random.permutation(jax.random.fold_in(rng, 2), count)]


def noise(own_key, extent, spread, reach, cuts=(), held_as=jnp.bfloat16):
    loudness = shard_levels(own_key, extent, cuts, -0.22, 0.18) if cuts else 1.0
    entries = jax.random.normal(own_key, extent, jnp.float32) * spread * loudness
    return jnp.minimum(jnp.maximum(entries, -reach), reach).astype(held_as)


def heavy_noise(key, shape, deviation, limit, cuts, heavy, kind=jnp.bfloat16):
    result = deviation * jax.random.normal(key, shape, jnp.float32)
    if cuts:
        result = result * shard_levels(key, shape, cuts, -0.22, 0.18)
    return jnp.clip(strengthened(result, jax.random.fold_in(key, 3), *heavy), -limit, limit).astype(kind)


def setup_inputs(seed: int = 0) -> dict:
    streams_of = jax.random.split(jax.random.key(seed), 7)
    grads = heavy_noise(streams_of[0], (N_DP, P_SIZE), 1.0, 6.0, ((0, 32),), (0, 1, 32, 2.75), jnp.float32)
    master = draw_master(jax.random.fold_in(streams_of[6], 71), 0)
    moment1 = noise(streams_of[2], (P_SIZE,), 0.5, 4.0, ((0, 32),), jnp.float32)
    moment2 = jnp.clip(jnp.exp(math.log(2.0) - 2.9957323 * jax.random.uniform(streams_of[3], (P_SIZE,), jnp.float32) ** shard_levels(streams_of[3], (P_SIZE,), ((0, 32),), -0.2, 0.2)), 0.1, 2.0)
    tensor_rows = uneven_parts(streams_of[4], NSEG, ROWS, ROWS // 2, 2).astype(jnp.int32)
    step_count = jax.random.randint(streams_of[5], (1,), 1, 20).astype(jnp.int32)
    return dict(grads=grads, master=master, moment1=moment1, moment2=moment2, tensor_rows=tensor_rows, step_count=step_count)


def reference(grads, master, moment1, moment2, tensor_rows, step_count):
    grad = lax.optimization_barrier(jnp.sum(grads, axis=0)) / jnp.float32(N_DP)
    new_moment1 = 0.9 * moment1 + 0.1 * grad
    new_moment2 = 0.999 * moment2 + 0.001 * grad * grad
    steps = step_count[0].astype(jnp.float32)
    first = new_moment1 / (1.0 - jnp.power(jnp.float32(0.9), steps))
    second = new_moment2 / (1.0 - jnp.power(jnp.float32(0.999), steps))
    update = first / (jnp.sqrt(second) + 1e-06) + 0.1 * master
    ends = jnp.cumsum(tensor_rows).astype(jnp.int32)
    starts = ends - tensor_rows
    row_index = jnp.arange(ROWS, dtype=jnp.int32)
    onehot = ((row_index[:, None] >= starts[None, :]) & (row_index[:, None] < ends[None, :])).astype(jnp.float32)
    weight_rows = master.reshape(ROWS, D)
    update_rows = update.reshape(ROWS, D)
    row_wsq = lax.optimization_barrier(jnp.sum(weight_rows * weight_rows, axis=1))
    row_usq = lax.optimization_barrier(jnp.sum(update_rows * update_rows, axis=1))
    wsq = lax.optimization_barrier(jnp.sum(onehot * row_wsq[:, None], axis=0))
    usq = lax.optimization_barrier(jnp.sum(onehot * row_usq[:, None], axis=0))
    ratio = jnp.sqrt(wsq / (usq + 1e-06))
    row_ratio = lax.optimization_barrier(jnp.sum(onehot * ratio[None, :], axis=1))
    new_master = (weight_rows - 0.2 * row_ratio[:, None] * update_rows).reshape(P_SIZE)
    new_weights = new_master.astype(jnp.bfloat16)
    return (new_weights, new_master, new_moment1, new_moment2)
```

```python
import functools

import jax
import jax.numpy as jnp
import numpy as np
from jax import lax
from jax.experimental import pallas as pl
from jax.experimental.pallas import tpu as pltpu
from jax.sharding import PartitionSpec as P

LANES = 128
BETA1, BETA2 = 0.9, 0.999
STEP_BITS = 8


def levels(count):
    chips = count // 2
    bits = chips.bit_length() - 1
    plane = 1 << ((bits + 1) // 2)
    return chips // plane, plane


def flipped(value, mask):
    bit = 1
    while bit <= mask:
        if mask & bit:
            value = value + bit * (1 - 2 * (value // bit % 2))
        bit *= 2
    return value


def power(base, step):
    result = jnp.ones(step.shape, jnp.float32)
    for bit in range(STEP_BITS):
        factor = float(np.float32(float(np.float32(base)) ** (2**bit)))
        result = result * jnp.where((step // 2**bit) % 2 == 1, factor, 1.0)
    return result


def kernel(
    count, line, plane,
    grads, master, moment1, moment2, rows_in, step_ref,
    early, deltas, ratios, m1_new, m2_new, mine, kept,
    own, pair_send, pair_recv, plane_send, plane_recv,
    line_send, line_recv, state, grad_ref, wsums, usums, masks, wsq_ref, rows_ref,
    local_sem, send_sem, recv_sem, plane_ready, line_ready, turn,
):
    me = lax.axis_index("dp")
    core = me % 2
    xy = me // 2 % plane
    z = me // (2 * plane)
    partner = me + 1 - 2 * core
    far_first = list(range(line - 1, 0, -1))
    near_first = far_first[::-1]
    others = list(range(plane - 1, 0, -1))
    layers = far_first + [0]
    stops = [0] + near_first
    f32, bf16 = jnp.float32, jnp.bfloat16
    tensors = rows_ref.shape[0]

    def plane_peer(mask):
        return (z * plane + flipped(xy, mask)) * 2 + core

    def line_peer(mask):
        return (flipped(z, mask) * plane + xy) * 2 + core

    def signal(semaphore, peer):
        pl.semaphore_signal(semaphore, inc=1, device_id=(peer,), device_id_type=pl.DeviceIdType.MESH)

    barrier = pltpu.get_barrier_semaphore()
    signal(barrier, partner)
    for p in others:
        pl.when((core == 1) & (flipped(xy, p) > xy))(functools.partial(signal, barrier, plane_peer(p)))
    for k in far_first:
        pl.when(flipped(z, k) > z)(functools.partial(signal, barrier, line_peer(k)))

    def local(source, target, slot):
        copy = pltpu.make_async_copy(source, target, local_sem.at[slot])
        copy.start()
        return copy

    loads = {k: local(grads.at[flipped(z, k)], own.at[k], 2 + k) for k in layers}
    for i, part in enumerate((moment1, moment2, master)):
        local(part, state.at[core, i], 0)
    rows_load = local(rows_in, rows_ref, 1)

    def greet():
        pl.semaphore_wait(barrier, 1 + z + core * xy)
        for p in others:
            pl.when((core == 1) & (flipped(xy, p) < xy))(functools.partial(signal, plane_ready, plane_peer(p)))
        for k in far_first:
            pl.when(flipped(z, k) < z)(functools.partial(signal, line_ready.at[z], line_peer(k)))

    step = jnp.full((8, LANES), step_ref[0], jnp.int32)
    first_scale = 1.0 - power(BETA1, step)
    second_scale = 1.0 - power(BETA2, step)

    def update_of(first, second, weight):
        return (first / first_scale) / (jnp.sqrt(second / second_scale) + 1e-06) + 0.1 * weight

    def make_row():
        ref = state.at[core]
        pltpu.make_async_copy(ref, ref, local_sem.at[0]).wait()
        weight = state[core, 2]
        kept[...] = weight
        high = weight.astype(bf16)
        early[0, 0, core, 0] = high
        early[0, 0, core, 1] = (weight - high.astype(f32)).astype(bf16)
        early[0, 0, core, 2] = update_of(0.9 * state[core, 0], 0.999 * state[core, 1], weight).astype(bf16)

    send_slots, recv_slots = [{}, {}], [{("line", k): k - 1 for k in near_first}, {}]

    def remote(side, to, kind, key, source, target, peer):
        sender = send_slots[side].setdefault(kind, len(send_slots[side]))
        receiver = recv_slots[to].setdefault(key, len(recv_slots[to]))
        pltpu.make_async_remote_copy(
            src_ref=source, dst_ref=target,
            send_sem=send_sem.at[sender], recv_sem=recv_sem.at[receiver],
            device_id=(peer,), device_id_type=pl.DeviceIdType.MESH,
        ).start()

    def wait_for(semaphore, ref):
        pltpu.make_async_copy(ref, ref, semaphore).wait()

    def arrived(side, key, ref):
        slot = recv_slots[side].setdefault(key, len(recv_slots[side]))
        wait_for(recv_sem.at[slot], ref)

    def left(side, kind, ref):
        wait_for(send_sem.at[send_slots[side][kind]], ref)

    def place(k, p):
        return flipped(z, k), flipped(xy, p)

    def put_sums(sums, k, p, values):
        at = (flipped(z, k) * plane + flipped(xy, p)) * 2
        for side in range(2):
            total = jnp.sum(values[side] * values[side], axis=0)
            sums[pl.ds(at + side, 1), :] = jnp.sum(total, axis=0, keepdims=True)

    def tensor_masks():
        rows_load.wait()
        index = lax.broadcasted_iota(jnp.int32, (count, LANES), 0)
        start = jnp.int32(0)
        for k in range(tensors):
            end = start + rows_ref[k]
            masks[k] = ((index >= start) & (index < end)).astype(f32)
            start = end

    def squares(sums):
        values = sums[...]
        parts = [jnp.sum(masks[k] * values, axis=0, keepdims=True) for k in range(tensors)]
        return jnp.sum(jnp.concatenate(parts, axis=0), axis=1, keepdims=True)

    def weight_squares():
        wsq_ref[...] = jnp.broadcast_to(squares(wsums), wsq_ref.shape)

    def weight_sums(k, p):
        weight = early[k, p, :, 0].astype(f32) + early[k, p, :, 1].astype(f32)
        put_sums(wsums, k, p, weight)

    def update_sums(k, p):
        update = early[k, p, :, 2].astype(f32) + deltas[k, p].astype(f32)
        put_sums(usums, k, p, update)

    rest = pl.ds(1, plane - 1)
    later = pl.ds(1, line - 1)

    @pl.when(core == 0)
    def _():
        greet()
        make_row()
        row = early.at[0, 0, 0]
        remote(0, 1, "row", "row", row, row, partner)
        for k in layers:
            loads[k].wait()
            pair_send[k] = own[k].astype(bf16)
            remote(0, 1, "pair", ("pair", k), pair_send.at[k], pair_recv.at[k], partner)
        remote(0, 1, "state", "state", state.at[0], state.at[0], partner)
        tensor_masks()
        arrived(0, "row", early.at[0, 0, 1])

        def spread(k):
            for p in others:
                remote(0, 1, "plane", ("early", k), early.at[k, 0], early.at[k, p], plane_peer(p) + 1)

        pl.semaphore_wait(turn, 1)
        pl.when(z < line - 1)(functools.partial(spread, 0))
        for to in range(line):
            @pl.when(z != to)
            def _():
                pl.when(z < to)(functools.partial(pl.semaphore_wait, line_ready.at[to], 1))
                k = jnp.bitwise_xor(z, to)
                sender = send_slots[0].setdefault("line", len(send_slots[0]))
                pltpu.make_async_remote_copy(
                    src_ref=early.at[0, 0], dst_ref=early.at[k, 0],
                    send_sem=send_sem.at[sender], recv_sem=recv_sem.at[k - 1],
                    device_id=((to * plane + xy) * 2,), device_id_type=pl.DeviceIdType.MESH,
                ).start()

        @pl.when(z == line - 1)
        def _():
            pl.semaphore_wait(turn, 1)
            spread(0)


        weight_sums(0, 0)
        for k in near_first:
            arrived(0, ("line", k), early.at[k, 0])
            spread(k)
            remote(0, 1, "column", ("column", k), early.at[k, 0], early.at[k, 0], partner)
            weight_sums(k, 0)

        arrived(0, "grad", grad_ref.at[0])
        grad = grad_ref[0]
        new_m1 = 0.9 * state[0, 0] + 0.1 * grad
        new_m2 = 0.999 * state[0, 1] + 0.001 * grad * grad
        mine[...] = update_of(new_m1, new_m2, state[0, 2])
        m1_new[...] = new_m1
        m2_new[...] = new_m2
        left(0, "pair", pair_send)
        left(0, "row", row)
        left(0, "state", state.at[0])
        left(0, "line", early.at[later, 0])
        left(0, "plane", early.at[:, rest])
        left(0, "column", early.at[later, 0])
        pl.when(z < line - 1)(functools.partial(pl.semaphore_wait, turn, 1))
        for k in stops:
            arrived(0, ("early", k), early.at[k, rest])
            for p in range(1, plane):
                weight_sums(k, p)
        weight_squares()
        for k in stops:
            arrived(0, ("delta", k), deltas.at[k])
            for p in range(plane):
                update_sums(k, p)

    @pl.when(core == 1)
    def _():
        greet()
        make_row()
        row = early.at[0, 0, 1]
        remote(1, 0, "row", "row", row, row, partner)
        for turn_k, k in enumerate(layers):
            loads[k].wait()
            if turn_k == 0:
                pl.when(xy < plane - 1)(functools.partial(pl.semaphore_wait, plane_ready, plane - 1 - xy))
                signal(turn, partner)
            arrived(1, ("pair", k), pair_recv.at[k])
            for p in others:
                at = flipped(xy, p)
                plane_send[k, p - 1] = (own[k, at] + pair_recv[k, at].astype(f32)).astype(bf16)
                remote(1, 1, "plane", ("plane", k), plane_send.at[k, p - 1], plane_recv.at[k, p - 1], plane_peer(p))

        tensor_masks()

        def pass_early(k):
            arrived(1, ("early", k), early.at[k, rest])
            remote(1, 0, "early", ("early", k), early.at[k, rest], early.at[k, rest], partner)
            if k > 0:
                arrived(1, ("column", k), early.at[k, 0])

        def weigh(k):
            for p in range(plane):
                if (k, p) != (0, 0):
                    weight_sums(k, p)

        def plane_sum(k):
            arrived(1, ("plane", k), plane_recv.at[k])
            total = own[k, xy] + pair_recv[k, xy].astype(f32)
            for p in others:
                total = total + plane_recv[k, p - 1].astype(f32)
            return total

        for to in range(1, line):
            pl.when(z < to)(functools.partial(pl.semaphore_wait, line_ready.at[to], 1))
        for k in far_first:
            line_send[k - 1] = plane_sum(k).astype(bf16)
            remote(1, 1, "line", "line", line_send.at[k - 1], line_recv.at[k - 1], line_peer(k))
            if k == far_first[0]:
                signal(turn, partner)
        grad = plane_sum(0)
        arrived(1, "state", state.at[0])
        arrived(1, "row", early.at[0, 0, 0])
        arrived(1, "line", line_recv)
        for k in far_first:
            grad = grad + line_recv[k - 1].astype(f32)
        grad = grad / jnp.float32(count)
        new_m1 = 0.9 * state[:, 0] + 0.1 * grad
        new_m2 = 0.999 * state[:, 1] + 0.001 * grad * grad
        update = update_of(new_m1, new_m2, state[:, 2])
        deltas[0, 0] = (update - early[0, 0, :, 2].astype(f32)).astype(bf16)
        for k in far_first:
            remote(1, 1, "dline", ("dline", k), deltas.at[0, 0], deltas.at[k, 0], line_peer(k))

        def spread(k):
            for p in others:
                remote(1, 1, "dplane", ("dplane", k), deltas.at[k, 0], deltas.at[k, p], plane_peer(p))

        spread(0)
        grad_ref[...] = grad
        remote(1, 0, "grad", "grad", grad_ref.at[0], grad_ref.at[0], partner)
        mine[...] = update[1]
        m1_new[...] = new_m1[1]
        m2_new[...] = new_m2[1]
        weight_sums(0, 0)
        left(1, "row", row)
        left(1, "plane", plane_send)
        left(1, "line", line_send)
        for k in near_first:
            arrived(1, ("dline", k), deltas.at[k, 0])
            spread(k)
            if k == near_first[0]:
                pass_early(0)
        for k in stops:
            if k > 0:
                pass_early(k)
            weigh(k)
        weight_squares()
        for k in stops:
            arrived(1, ("dplane", k), deltas.at[k, rest])
            remote(1, 0, "delta", ("delta", k), deltas.at[k], deltas.at[k], partner)
            for p in range(plane):
                update_sums(k, p)
        left(1, "grad", grad_ref.at[0])
        left(1, "dline", deltas.at[later, 0])
        left(1, "dplane", deltas.at[:, rest])
        left(1, "delta", deltas)
        left(1, "early", early.at[:, rest])

    ratio = 0.2 * jnp.sqrt(wsq_ref[...] / (squares(usums) + 1e-06))
    row_ratio = masks[0] * ratio[0:1]
    for k in range(1, tensors):
        row_ratio = row_ratio + masks[k] * ratio[k:k + 1]
    ratios[...] = row_ratio
    assert max(map(len, send_slots)) <= send_sem.shape[0]
    assert max(map(len, recv_slots)) <= recv_sem.shape[0]


def finish(
    line, plane,
    early, deltas, ratios, m1_new, m2_new, mine, kept,
    weights_out, master_out, moment1_out, moment2_out,
    weights, master_new, sem,
):
    me = lax.axis_index("dp")
    z, xy, core = me // (2 * plane), me // 2 % plane, me % 2
    copies = [
        pltpu.make_async_copy(m1_new, moment1_out, sem.at[0]),
        pltpu.make_async_copy(m2_new, moment2_out, sem.at[1]),
    ]
    for copy in copies:
        copy.start()

    def scale(j, at, side):
        return ratios[pl.ds((j * plane + at) * 2 + side, 1), :]

    master_new[...] = kept[...] - scale(z, xy, core) * mine[...]
    copies.append(pltpu.make_async_copy(master_new, master_out, sem.at[2]))
    copies[-1].start()

    def layer_copy(j):
        return pltpu.make_async_copy(weights.at[j], weights_out.at[j], sem.at[3 + j])

    @pl.loop(0, line)
    def _(k):
        j = jnp.bitwise_xor(z, k)
        for p in range(plane):
            at = flipped(xy, p)
            for side in range(2):
                high, low, guess = (early[k, p, side, i].astype(jnp.float32) for i in range(3))
                update = guess + deltas[k, p, side].astype(jnp.float32)
                new_row = (high + low) - scale(j, at, side) * update
                weights[j, at, side] = new_row.astype(jnp.bfloat16)
        layer_copy(j).start()

    for j in range(line):
        copies.append(layer_copy(j))
    for copy in copies:
        copy.wait()


def pinned(array):
    return pltpu.with_memory_space_constraint(array, pltpu.HBM)


def body(grads, master, moment1, moment2, tensor_rows, step_count):
    count = lax.axis_size("dp")
    line, plane = levels(count)
    row = (master.shape[0] // (8 * LANES), 8, LANES)
    f32, bf16 = jnp.float32, jnp.bfloat16
    hbm = pl.BlockSpec(memory_space=pltpu.HBM)
    vmem = pl.BlockSpec(memory_space=pltpu.VMEM)
    pair = (2,) + row
    table = (line, plane) + pair
    kept = jax.ShapeDtypeStruct(row, f32)
    state = pl.pallas_call(
        functools.partial(kernel, count, line, plane),
        out_shape=(
            jax.ShapeDtypeStruct((line, plane, 2, 3) + row, bf16),
            jax.ShapeDtypeStruct(table, bf16),
            jax.ShapeDtypeStruct((count, LANES), f32),
            kept, kept, kept, kept,
        ),
        in_specs=[hbm] * 5 + [pl.BlockSpec(memory_space=pltpu.SMEM)],
        out_specs=(vmem,) * 7,
        scratch_shapes=[
            pltpu.VMEM(table, f32),
            pltpu.VMEM(table, bf16),
            pltpu.VMEM(table, bf16),
            pltpu.VMEM((line, plane - 1) + pair, bf16),
            pltpu.VMEM((line, plane - 1) + pair, bf16),
            pltpu.VMEM((line - 1,) + pair, bf16),
            pltpu.VMEM((line - 1,) + pair, bf16),
            pltpu.VMEM((2, 3) + row, f32),
            pltpu.VMEM(pair, f32),
            pltpu.VMEM((count, LANES), f32),
            pltpu.VMEM((count, LANES), f32),
            pltpu.VMEM((tensor_rows.shape[0], count, LANES), f32),
            pltpu.VMEM((tensor_rows.shape[0], LANES), f32),
            pltpu.SMEM(tensor_rows.shape, jnp.int32),
            pltpu.SemaphoreType.DMA((line + 2,)),
            pltpu.SemaphoreType.DMA((8,)),
            pltpu.SemaphoreType.DMA((6 * line + 1,)),
            pltpu.SemaphoreType.REGULAR,
            pltpu.SemaphoreType.REGULAR((line,)),
            pltpu.SemaphoreType.REGULAR,
        ],
        compiler_params=pltpu.CompilerParams(
            collective_id=0, has_side_effects=True, vmem_limit_bytes=48 * 1024 * 1024
        ),
        name="exchange",
    )(
        pinned(grads.reshape(table)),
        pinned(master.reshape(row)), pinned(moment1.reshape(row)), pinned(moment2.reshape(row)),
        pinned(tensor_rows), step_count,
    )
    outs = pl.pallas_call(
        functools.partial(finish, line, plane),
        out_shape=(jax.ShapeDtypeStruct(table, bf16), kept, kept, kept),
        in_specs=[vmem] * 7,
        out_specs=(hbm,) * 4,
        scratch_shapes=[
            pltpu.VMEM(table, bf16),
            pltpu.VMEM(row, f32),
            pltpu.SemaphoreType.DMA((3 + line,)),
        ],
        compiler_params=pltpu.CompilerParams(vmem_limit_bytes=24 * 1024 * 1024),
        name="finish",
    )(*state)
    return tuple(out.reshape(-1) for out in outs)


def solution(mesh):
    placed = (P("dp", None), P("dp"), P("dp"), P("dp"), P(), P())
    return jax.shard_map(
        body,
        mesh=mesh,
        in_specs=placed,
        out_specs=(P(), P("dp"), P("dp"), P("dp")),
        check_vma=False,
    )
```

```python
import functools
import math

import jax
import jax.numpy as jnp
import numpy as np
from jax import lax
from jax.experimental import pallas as pl
from jax.experimental.pallas import tpu as pltpu
from jax.sharding import PartitionSpec as P

LANES = 128
BETA1, BETA2 = 0.9, 0.999
STEP_BITS = 8


def levels(count):
    chips = count // 2
    bits = chips.bit_length() - 1
    plane = 1 << ((bits + 1) // 2)
    return chips // plane, plane


def flipped(value, mask):
    bit = 1
    while bit <= mask:
        if mask & bit:
            value = value + bit * (1 - 2 * (value // bit % 2))
        bit *= 2
    return value


def power(base, step):
    result = jnp.ones(step.shape, jnp.float32)
    for bit in range(STEP_BITS):
        factor = float(np.float32(float(np.float32(base)) ** (2**bit)))
        result = result * jnp.where((step // 2**bit) % 2 == 1, factor, 1.0)
    return result


def kernel(
    count, line, plane,
    grads, master, moment1, moment2, rows_in, step_ref,
    weights, updates, ratios, m1_new, m2_new, mine, kept,
    early, deltas, leaving, own, pair_send, pair_recv, plane_send, plane_recv,
    line_send, line_recv, state, grad_ref, wsums, usums, masks, wsq_ref, rows_ref,
    sems, plane_ready, line_ready, turn,
):
    me = lax.axis_index("dp")
    core = me % 2
    xy = me // 2 % plane
    z = me // (2 * plane)
    partner = me + 1 - 2 * core
    far_first = list(range(line - 1, 0, -1))
    near_first = far_first[::-1]
    others = list(range(plane - 1, 0, -1))
    order = sorted(near_first, key=lambda k: (bin(k).count("1"), -k))
    layers = order + [0]
    stops = [0] + near_first
    f32, bf16 = jnp.float32, jnp.bfloat16
    tensors = rows_ref.shape[0]

    def plane_peer(mask):
        return (z * plane + flipped(xy, mask)) * 2 + core

    def line_peer(mask):
        return (flipped(z, mask) * plane + xy) * 2 + core

    def signal(semaphore, peer):
        pl.semaphore_signal(semaphore, inc=1, device_id=(peer,), device_id_type=pl.DeviceIdType.MESH)

    barrier = pltpu.get_barrier_semaphore()
    signal(barrier, partner)
    for p in others:
        pl.when((core == 1) & (flipped(xy, p) > xy))(functools.partial(signal, barrier, plane_peer(p)))
    for k in far_first:
        pl.when(flipped(z, k) > z)(functools.partial(signal, barrier, line_peer(k)))

    def local(source, target, slot):
        copy = pltpu.make_async_copy(source, target, sems.at[slot])
        copy.start()
        return copy

    loads = {k: local(grads.at[flipped(z, k)], own.at[k], k) for k in layers}
    for i, part in enumerate((moment1, moment2, master)):
        local(part, state.at[core, i], 4 * line + 2)
    rows_load = local(rows_in, rows_ref, 4 * line + 3)

    def greet():
        pl.semaphore_wait(barrier, 1 + z + core * xy)
        for p in others:
            pl.when((core == 1) & (flipped(xy, p) < xy))(functools.partial(signal, plane_ready, plane_peer(p)))
        for k in far_first:
            pl.when(flipped(z, k) < z)(functools.partial(signal, line_ready.at[z - 1], line_peer(k)))

    step = jnp.full((8, LANES), step_ref[0], jnp.int32)
    first_scale = 1.0 - power(BETA1, step)
    second_scale = 1.0 - power(BETA2, step)

    def update_of(first, second, weight):
        return (first / first_scale) / (jnp.sqrt(second / second_scale) + 1e-06) + 0.1 * weight

    def make_row():
        ref = state.at[core]
        pltpu.make_async_copy(ref, ref, sems.at[4 * line + 2]).wait()
        weight = state[core, 2]
        kept[...] = weight
        high = weight.astype(bf16)
        early[0, 0, core, 0] = high
        early[0, 0, core, 1] = (weight - high.astype(f32)).astype(bf16)
        early[0, 0, core, 2] = update_of(0.9 * state[core, 0], 0.999 * state[core, 1], weight).astype(bf16)

    pools = {
        0: {"row": 2 * line, "grad": 3 * line, "delta": 0, "early": line, "line": 2 * line},
        1: {"row": 4 * line + 1, "state": 4 * line + 1, "line": 4 * line, "pair": line, "plane": 2 * line,
            "dplane": 0, "dline": line, "early": 3 * line},
    }
    sent = [0, 0]

    def remote(side, to, key, source, target, peer):
        name, k = key if isinstance(key, tuple) else (key, 0)
        pltpu.make_async_remote_copy(
            src_ref=source, dst_ref=target,
            send_sem=sems.at[4 * line + 4], recv_sem=sems.at[pools[to][name] + k],
            device_id=(peer,), device_id_type=pl.DeviceIdType.MESH,
        ).start()
        words = 2 if source.dtype == f32 else 1
        sent[side] += words * math.prod(source.shape[:-3])

    def wait_for(semaphore, ref):
        pltpu.make_async_copy(ref, ref, semaphore).wait()

    def arrived(side, key, ref):
        name, k = key if isinstance(key, tuple) else (key, 0)
        wait_for(sems.at[pools[side][name] + k], ref)

    def all_left(side):
        wait_for(sems.at[4 * line + 4], leaving.at[pl.ds(0, sent[side])])

    def place(k, p):
        return flipped(z, k), flipped(xy, p)

    def put_sums(sums, k, p, values):
        at = (flipped(z, k) * plane + flipped(xy, p)) * 2
        for side in range(2):
            total = jnp.sum(values[side] * values[side], axis=0)
            sums[pl.ds(at + side, 1), :] = jnp.sum(total, axis=0, keepdims=True)

    def tensor_masks():
        rows_load.wait()
        index = lax.broadcasted_iota(jnp.int32, (count, LANES), 0)
        start = jnp.int32(0)
        for k in range(tensors):
            end = start + rows_ref[k]
            masks[k] = ((index >= start) & (index < end)).astype(f32)
            start = end

    def squares(sums):
        values = sums[...]
        parts = [jnp.sum(masks[k] * values, axis=0, keepdims=True) for k in range(tensors)]
        return jnp.sum(jnp.concatenate(parts, axis=0), axis=1, keepdims=True)

    def weight_squares():
        wsq_ref[...] = jnp.broadcast_to(squares(wsums), wsq_ref.shape)

    def weight_sums(k, p):
        weight = early[k, p, :, 0].astype(f32) + early[k, p, :, 1].astype(f32)
        weights[place(k, p)] = weight
        put_sums(wsums, k, p, weight)

    def update_sums(k, p):
        update = early[k, p, :, 2].astype(f32) + deltas[k, p].astype(f32)
        updates[place(k, p)] = update
        put_sums(usums, k, p, update)

    rest = pl.ds(1, plane - 1)
    later = pl.ds(1, line - 1)

    @pl.when(core == 0)
    def _():
        greet()
        make_row()
        row = early.at[0, 0, 0]
        remote(0, 1, "row", row, row, partner)
        for k in layers:
            loads[k].wait()
            pair_send[k] = own[k].astype(bf16)
            remote(0, 1, ("pair", k), pair_send.at[k], pair_recv.at[k], partner)
        remote(0, 1, "state", state.at[0], state.at[0], partner)
        tensor_masks()
        arrived(0, "row", early.at[0, 0, 1])

        def spread(k):
            for p in others:
                remote(0, 1, ("early", k), early.at[k, 0], early.at[k, p], plane_peer(p) + 1)

        for to in range(line):
            @pl.when(z != to)
            def _():
                if to > 0:
                    pl.when(z < to)(functools.partial(pl.semaphore_wait, line_ready.at[to - 1], 1))
                k = jnp.bitwise_xor(z, to)
                remote(0, 0, ("line", k), early.at[0, 0], early.at[k, 0], (to * plane + xy) * 2)

        sent[0] -= math.prod(early.shape[2:4])

        pl.semaphore_wait(turn, 1)
        spread(0)
        weight_sums(0, 0)
        for k in near_first:
            arrived(0, ("line", k), early.at[k, 0])
            spread(k)
            remote(0, 1, ("early", k), early.at[k, 0], early.at[k, 0], partner)
            weight_sums(k, 0)

        arrived(0, "grad", grad_ref.at[0])
        grad = grad_ref[0]
        new_m1 = 0.9 * state[0, 0] + 0.1 * grad
        new_m2 = 0.999 * state[0, 1] + 0.001 * grad * grad
        mine[...] = update_of(new_m1, new_m2, state[0, 2])
        m1_new[...] = new_m1
        m2_new[...] = new_m2
        for k in stops:
            arrived(0, ("early", k), early.at[k, rest])
            for p in range(1, plane):
                weight_sums(k, p)
        weight_squares()
        for k in stops:
            arrived(0, ("delta", k), deltas.at[k])
            for p in range(plane):
                update_sums(k, p)
        all_left(0)

    @pl.when(core == 1)
    def _():
        greet()
        make_row()
        row = early.at[0, 0, 1]
        remote(1, 0, "row", row, row, partner)
        for turn_k, k in enumerate(layers):
            loads[k].wait()
            if turn_k == 0:
                pl.when(xy < plane - 1)(functools.partial(pl.semaphore_wait, plane_ready, plane - 1 - xy))
            arrived(1, ("pair", k), pair_recv.at[k])
            for p in others:
                at = flipped(xy, p)
                plane_send[k, p - 1] = (own[k, at] + pair_recv[k, at].astype(f32)).astype(bf16)
                remote(1, 1, ("plane", k), plane_send.at[k, p - 1], plane_recv.at[k, p - 1], plane_peer(p))

        tensor_masks()

        def pass_early(k):
            arrived(1, ("early", k), early.at[k] if k > 0 else early.at[k, rest])
            remote(1, 0, ("early", k), early.at[k, rest], early.at[k, rest], partner)

        def weigh(k):
            for p in range(plane):
                if (k, p) != (0, 0):
                    weight_sums(k, p)

        def plane_sum(k):
            arrived(1, ("plane", k), plane_recv.at[k])
            total = own[k, xy] + pair_recv[k, xy].astype(f32)
            for p in others:
                total = total + plane_recv[k, p - 1].astype(f32)
            return total

        for to in range(1, line):
            pl.when(z < to)(functools.partial(pl.semaphore_wait, line_ready.at[to - 1], 1))
        for k in order:
            line_send[k - 1] = plane_sum(k).astype(bf16)
            remote(1, 1, "line", line_send.at[k - 1], line_recv.at[k - 1], line_peer(k))
            if k == order[0]:
                signal(turn, partner)
        grad = plane_sum(0)
        arrived(1, "row", early.at[0, pl.ds(0, 3), 0])
        arrived(1, "line", line_recv)
        for k in far_first:
            grad = grad + line_recv[k - 1].astype(f32)
        grad = grad / jnp.float32(count)
        new_m1 = 0.9 * state[:, 0] + 0.1 * grad
        new_m2 = 0.999 * state[:, 1] + 0.001 * grad * grad
        update = update_of(new_m1, new_m2, state[:, 2])
        deltas[0, 0] = (update - early[0, 0, :, 2].astype(f32)).astype(bf16)
        for k in far_first:
            remote(1, 1, ("dline", k), deltas.at[0, 0], deltas.at[k, 0], line_peer(k))

        def spread(k):
            for p in others:
                remote(1, 1, ("dplane", k), deltas.at[k, 0], deltas.at[k, p], plane_peer(p))

        spread(0)
        grad_ref[...] = grad
        remote(1, 0, "grad", grad_ref.at[0], grad_ref.at[0], partner)
        mine[...] = update[1]
        m1_new[...] = new_m1[1]
        m2_new[...] = new_m2[1]
        weight_sums(0, 0)
        for k in near_first:
            arrived(1, ("dline", k), deltas.at[k, 0])
            spread(k)
            if k == near_first[0]:
                pass_early(0)
        for k in stops:
            if k > 0:
                pass_early(k)
            weigh(k)
        weight_squares()
        for k in stops:
            arrived(1, ("dplane", k), deltas.at[k, rest])
            remote(1, 0, ("delta", k), deltas.at[k], deltas.at[k], partner)
            for p in range(plane):
                update_sums(k, p)
        all_left(1)

    ratio = 0.2 * jnp.sqrt(wsq_ref[...] / (squares(usums) + 1e-06))
    row_ratio = masks[0] * ratio[0:1]
    for k in range(1, tensors):
        row_ratio = row_ratio + masks[k] * ratio[k:k + 1]
    ratios[...] = row_ratio


def finish(
    line, plane,
    weights, updates, ratios, m1_new, m2_new, mine, kept,
    weights_out, master_out, moment1_out, moment2_out,
    rounded, master_new, sem,
):
    me = lax.axis_index("dp")
    copies = [
        pltpu.make_async_copy(m1_new, moment1_out, sem.at[0]),
        pltpu.make_async_copy(m2_new, moment2_out, sem.at[1]),
    ]
    for copy in copies:
        copy.start()
    master_new[...] = kept[...] - ratios[pl.ds(me, 1), :] * mine[...]
    copies.append(pltpu.make_async_copy(master_new, master_out, sem.at[2]))
    copies[-1].start()

    def layer_copy(j):
        return pltpu.make_async_copy(rounded.at[j], weights_out.at[j], sem.at[3 + j])

    @pl.loop(0, line)
    def _(j):
        for at in range(plane):
            for side in range(2):
                scale = ratios[pl.ds((j * plane + at) * 2 + side, 1), :]
                new_row = weights[j, at, side] - scale * updates[j, at, side]
                rounded[j, at, side] = new_row.astype(jnp.bfloat16)
        layer_copy(j).start()

    for j in range(line):
        copies.append(layer_copy(j))
    for copy in copies:
        copy.wait()


def pinned(array):
    return pltpu.with_memory_space_constraint(array, pltpu.HBM)


def body(grads, master, moment1, moment2, tensor_rows, step_count):
    count = lax.axis_size("dp")
    line, plane = levels(count)
    row = (master.shape[0] // (8 * LANES), 8, LANES)
    f32, bf16 = jnp.float32, jnp.bfloat16
    hbm = pl.BlockSpec(memory_space=pltpu.HBM)
    vmem = pl.BlockSpec(memory_space=pltpu.VMEM)
    pair = (2,) + row
    table = (line, plane) + pair
    kept = jax.ShapeDtypeStruct(row, f32)
    leaving = 12 * line * plane
    state = pl.pallas_call(
        functools.partial(kernel, count, line, plane),
        out_shape=(
            jax.ShapeDtypeStruct(table, f32),
            jax.ShapeDtypeStruct(table, f32),
            jax.ShapeDtypeStruct((count, LANES), f32),
            kept, kept, kept, kept,
        ),
        in_specs=[hbm] * 5 + [pl.BlockSpec(memory_space=pltpu.SMEM)],
        out_specs=(vmem,) * 7,
        scratch_shapes=[
            pltpu.VMEM((line, plane, 2, 3) + row, bf16),
            pltpu.VMEM(table, bf16),
            pltpu.VMEM((leaving,) + row, bf16),
            pltpu.VMEM(table, f32),
            pltpu.VMEM(table, bf16),
            pltpu.VMEM(table, bf16),
            pltpu.VMEM((line, plane - 1) + pair, bf16),
            pltpu.VMEM((line, plane - 1) + pair, bf16),
            pltpu.VMEM((line - 1,) + pair, bf16),
            pltpu.VMEM((line - 1,) + pair, bf16),
            pltpu.VMEM((2, 3) + row, f32),
            pltpu.VMEM(pair, f32),
            pltpu.VMEM((count, LANES), f32),
            pltpu.VMEM((count, LANES), f32),
            pltpu.VMEM((tensor_rows.shape[0], count, LANES), f32),
            pltpu.VMEM((tensor_rows.shape[0], LANES), f32),
            pltpu.SMEM(tensor_rows.shape, jnp.int32),
            pltpu.SemaphoreType.DMA((4 * line + 5,)),
            pltpu.SemaphoreType.REGULAR,
            pltpu.SemaphoreType.REGULAR((line - 1,)),
            pltpu.SemaphoreType.REGULAR,
        ],
        compiler_params=pltpu.CompilerParams(
            collective_id=0, has_side_effects=True, vmem_limit_bytes=min(60, 20 + count // 4) * 1024 * 1024
        ),
        name="exchange",
    )(
        pinned(grads.reshape(table)),
        pinned(master.reshape(row)), pinned(moment1.reshape(row)), pinned(moment2.reshape(row)),
        pinned(tensor_rows), step_count,
    )
    outs = pl.pallas_call(
        functools.partial(finish, line, plane),
        out_shape=(jax.ShapeDtypeStruct(table, bf16), kept, kept, kept),
        in_specs=[vmem] * 7,
        out_specs=(hbm,) * 4,
        scratch_shapes=[
            pltpu.VMEM(table, bf16),
            pltpu.VMEM(row, f32),
            pltpu.SemaphoreType.DMA((3 + line,)),
        ],
        compiler_params=pltpu.CompilerParams(vmem_limit_bytes=24 * 1024 * 1024),
        name="finish",
    )(*state)
    return tuple(out.reshape(-1) for out in outs)


def solution(mesh):
    placed = (P("dp", None), P("dp"), P("dp"), P("dp"), P(), P())
    return jax.shard_map(
        body,
        mesh=mesh,
        in_specs=placed,
        out_specs=(P(), P("dp"), P("dp"), P("dp")),
        check_vma=False,
    )
```

```python
import functools
import math

import jax
import jax.numpy as jnp
import numpy as np
from jax import lax
from jax.experimental import pallas as pl
from jax.experimental.pallas import tpu as pltpu
from jax.sharding import PartitionSpec as P

LANES = 128
BETA1, BETA2 = 0.9, 0.999
STEP_BITS = 8


def levels(count):
    chips = count // 2
    bits = chips.bit_length() - 1
    plane = 1 << ((bits + 1) // 2)
    return chips // plane, plane


def flipped(value, mask):
    bit = 1
    while bit <= mask:
        if mask & bit:
            value = value + bit * (1 - 2 * (value // bit % 2))
        bit *= 2
    return value


def power(base, step):
    result = jnp.ones(step.shape, jnp.float32)
    for bit in range(STEP_BITS):
        factor = float(np.float32(float(np.float32(base)) ** (2**bit)))
        result = result * jnp.where((step // 2**bit) % 2 == 1, factor, 1.0)
    return result


def kernel(
    count, line, plane,
    grads, master, moment1, moment2, rows_in, step_ref,
    weights, updates, ratios, m1_new, m2_new, mine, kept,
    early, deltas, leaving, own, pair_send, pair_recv, plane_send, plane_recv,
    line_send, line_recv, state, grad_ref, wsums, usums, masks, wsq_ref, rows_ref,
    sems, plane_ready, line_ready, turn,
):
    me = lax.axis_index("dp")
    core = me % 2
    xy = me // 2 % plane
    z = me // (2 * plane)
    partner = me + 1 - 2 * core
    far_first = list(range(line - 1, 0, -1))
    near_first = far_first[::-1]
    others = list(range(plane - 1, 0, -1))
    order = sorted(near_first, key=lambda k: (bin(k).count("1"), -k))
    layers = order + [0]
    stops = [0] + near_first
    far = list(range(line // 2, line))
    f32, bf16 = jnp.float32, jnp.bfloat16
    tensors = rows_ref.shape[0]

    def plane_peer(mask):
        return (z * plane + flipped(xy, mask)) * 2 + core

    def line_peer(mask):
        return (flipped(z, mask) * plane + xy) * 2 + core

    def signal(semaphore, peer):
        pl.semaphore_signal(semaphore, inc=1, device_id=(peer,), device_id_type=pl.DeviceIdType.MESH)

    barrier = pltpu.get_barrier_semaphore()
    signal(barrier, partner)
    for p in others:
        pl.when((core == 1) & (flipped(xy, p) > xy))(functools.partial(signal, barrier, plane_peer(p)))
    for k in far_first:
        pl.when(flipped(z, k) > z)(functools.partial(signal, barrier, line_peer(k)))

    def local(source, target, slot):
        copy = pltpu.make_async_copy(source, target, sems.at[slot])
        copy.start()
        return copy

    loads = {k: local(grads.at[flipped(z, k)], own.at[k], k) for k in layers}
    for i, part in enumerate((moment1, moment2, master)):
        local(part, state.at[core, i], 4 * line + 2)
    rows_load = local(rows_in, rows_ref, 4 * line + 3)

    def greet():
        pl.semaphore_wait(barrier, 1 + z + core * xy)
        for p in others:
            pl.when((core == 1) & (flipped(xy, p) < xy))(functools.partial(signal, plane_ready, plane_peer(p)))
        for k in far_first:
            pl.when(flipped(z, k) < z)(functools.partial(signal, line_ready.at[z - 1], line_peer(k)))

    step = jnp.full((8, LANES), step_ref[0], jnp.int32)
    first_scale = 1.0 - power(BETA1, step)
    second_scale = 1.0 - power(BETA2, step)

    def update_of(first, second, weight):
        return (first / first_scale) / (jnp.sqrt(second / second_scale) + 1e-06) + 0.1 * weight

    def make_row():
        ref = state.at[core]
        pltpu.make_async_copy(ref, ref, sems.at[4 * line + 2]).wait()
        weight = state[core, 2]
        kept[...] = weight
        high = weight.astype(bf16)
        early[0, 0, core, 0] = high
        early[0, 0, core, 1] = (weight - high.astype(f32)).astype(bf16)
        early[0, 0, core, 2] = update_of(0.9 * state[core, 0], 0.999 * state[core, 1], weight).astype(bf16)

    pools = {
        0: {"row": 2 * line, "grad": 3 * line, "delta": 0, "early": line, "line": 2 * line},
        1: {"row": 4 * line + 1, "state": 4 * line + 1, "line": 4 * line, "pair": line, "plane": 2 * line,
            "dplane": 0, "dline": line, "early": 3 * line},
    }
    sent = [0, 0]

    def remote(side, to, key, source, target, peer):
        name, k = key if isinstance(key, tuple) else (key, 0)
        pltpu.make_async_remote_copy(
            src_ref=source, dst_ref=target,
            send_sem=sems.at[4 * line + 4], recv_sem=sems.at[pools[to][name] + k],
            device_id=(peer,), device_id_type=pl.DeviceIdType.MESH,
        ).start()
        words = 2 if source.dtype == f32 else 1
        sent[side] += words * math.prod(source.shape[:-3])

    def wait_for(semaphore, ref):
        pltpu.make_async_copy(ref, ref, semaphore).wait()

    def arrived(side, key, ref):
        name, k = key if isinstance(key, tuple) else (key, 0)
        wait_for(sems.at[pools[side][name] + k], ref)

    def all_left(side):
        wait_for(sems.at[4 * line + 4], leaving.at[pl.ds(0, sent[side])])

    def place(k, p):
        return flipped(z, k), flipped(xy, p)

    def put_sums(sums, k, p, values):
        at = (flipped(z, k) * plane + flipped(xy, p)) * 2
        for side in range(2):
            total = jnp.sum(values[side] * values[side], axis=0)
            sums[pl.ds(at + side, 1), :] = jnp.sum(total, axis=0, keepdims=True)

    def tensor_masks():
        rows_load.wait()
        index = lax.broadcasted_iota(jnp.int32, (count, LANES), 0)
        start = jnp.int32(0)
        for k in range(tensors):
            end = start + rows_ref[k]
            masks[k] = ((index >= start) & (index < end)).astype(f32)
            start = end

    def squares(sums):
        values = sums[...]
        parts = [jnp.sum(masks[k] * values, axis=0, keepdims=True) for k in range(tensors)]
        return jnp.sum(jnp.concatenate(parts, axis=0), axis=1, keepdims=True)

    def weight_squares():
        wsq_ref[...] = jnp.broadcast_to(squares(wsums), wsq_ref.shape)

    def weight_sums(k, p):
        weight = early[k, p, :, 0].astype(f32) + early[k, p, :, 1].astype(f32)
        weights[place(k, p)] = weight
        put_sums(wsums, k, p, weight)

    def update_sums(k, p):
        update = early[k, p, :, 2].astype(f32) + deltas[k, p].astype(f32)
        updates[place(k, p)] = update
        put_sums(usums, k, p, update)

    rest = pl.ds(1, plane - 1)
    later = pl.ds(1, line - 1)

    @pl.when(core == 0)
    def _():
        greet()
        make_row()
        row = early.at[0, 0, 0]
        remote(0, 1, "row", row, row, partner)
        for k in layers:
            loads[k].wait()
            pair_send[k] = own[k].astype(bf16)
            remote(0, 1, ("pair", k), pair_send.at[k], pair_recv.at[k], partner)
        remote(0, 1, "state", state.at[0], state.at[0], partner)
        tensor_masks()
        arrived(0, "row", early.at[0, 0, 1])

        def spread(k):
            for p in others:
                remote(0, 1, ("early", k), early.at[k, 0], early.at[k, p], plane_peer(p) + 1)

        for to in range(line):
            @pl.when(z != to)
            def _():
                if to > 0:
                    pl.when(z < to)(functools.partial(pl.semaphore_wait, line_ready.at[to - 1], 1))
                k = jnp.bitwise_xor(z, to)
                remote(0, 0, ("line", k), early.at[0, 0], early.at[k, 0], (to * plane + xy) * 2)

        sent[0] -= math.prod(early.shape[2:4])

        pl.semaphore_wait(turn, 1)
        spread(0)
        weight_sums(0, 0)
        for k in near_first:
            arrived(0, ("line", k), early.at[k, 0])
            spread(k)
            remote(0, 1, ("early", k), early.at[k, 0], early.at[k, 0], partner)
            weight_sums(k, 0)

        arrived(0, "grad", grad_ref.at[0])
        grad = grad_ref[0]
        new_m1 = 0.9 * state[0, 0] + 0.1 * grad
        new_m2 = 0.999 * state[0, 1] + 0.001 * grad * grad
        mine[...] = update_of(new_m1, new_m2, state[0, 2])
        m1_new[...] = new_m1
        m2_new[...] = new_m2
        for k in stops:
            arrived(0, ("early", k), early.at[k, rest])
            for p in range(1, plane):
                weight_sums(k, p)
        weight_squares()
        for k in stops:
            arrived(0, ("delta", k), deltas.at[k])
            for p in range(plane):
                update_sums(k, p)
        all_left(0)

    @pl.when(core == 1)
    def _():
        greet()
        make_row()
        row = early.at[0, 0, 1]
        remote(1, 0, "row", row, row, partner)
        for turn_k, k in enumerate(layers):
            loads[k].wait()
            if turn_k == 0:
                pl.when(xy < plane - 1)(functools.partial(pl.semaphore_wait, plane_ready, plane - 1 - xy))
            arrived(1, ("pair", k), pair_recv.at[k])
            for p in others:
                at = flipped(xy, p)
                plane_send[k, p - 1] = (own[k, at] + pair_recv[k, at].astype(f32)).astype(bf16)
                remote(1, 1, ("plane", k), plane_send.at[k, p - 1], plane_recv.at[k, p - 1], plane_peer(p))

        tensor_masks()
        all_left(1)
        sent[1] = 0
        signal(turn, partner)

        def pass_early(k):
            arrived(1, ("early", k), early.at[k] if k > 0 else early.at[k, rest])
            remote(1, 0, ("early", k), early.at[k, rest], early.at[k, rest], partner)

        def weigh(k):
            for p in range(plane):
                if (k, p) != (0, 0):
                    weight_sums(k, p)

        def plane_sum(k):
            arrived(1, ("plane", k), plane_recv.at[k])
            total = own[k, xy] + pair_recv[k, xy].astype(f32)
            for p in others:
                total = total + plane_recv[k, p - 1].astype(f32)
            return total

        for to in range(1, line):
            pl.when(z < to)(functools.partial(pl.semaphore_wait, line_ready.at[to - 1], 1))
        for k in order:
            line_send[k - 1] = plane_sum(k).astype(bf16)
            remote(1, 1, "line", line_send.at[k - 1], line_recv.at[k - 1], line_peer(k))
        grad = plane_sum(0)
        arrived(1, "row", early.at[0, pl.ds(0, 3), 0])
        arrived(1, "line", line_recv)
        for k in far_first:
            grad = grad + line_recv[k - 1].astype(f32)
        grad = grad / jnp.float32(count)
        new_m1 = 0.9 * state[:, 0] + 0.1 * grad
        new_m2 = 0.999 * state[:, 1] + 0.001 * grad * grad
        update = update_of(new_m1, new_m2, state[:, 2])
        deltas[0, 0] = (update - early[0, 0, :, 2].astype(f32)).astype(bf16)
        for k in far_first:
            remote(1, 1, ("dline", k), deltas.at[0, 0], deltas.at[k, 0], line_peer(k))

        def spread(k):
            for p in others:
                remote(1, 1, ("dplane", k), deltas.at[k, 0], deltas.at[k, p], plane_peer(p))

        def spread_both(k):
            for p in others:
                remote(1, 0, ("delta", k), deltas.at[k, 0], deltas.at[k, p], plane_peer(p) - 1)
            remote(1, 0, ("delta", k), deltas.at[k, 0], deltas.at[k, 0], partner)

        spread(0)
        grad_ref[...] = grad
        remote(1, 0, "grad", grad_ref.at[0], grad_ref.at[0], partner)
        mine[...] = update[1]
        m1_new[...] = new_m1[1]
        m2_new[...] = new_m2[1]
        weight_sums(0, 0)
        for turn_k, of in enumerate(near_first + [0]):
            @pl.when(z != of)
            def _():
                k = jnp.bitwise_xor(z, of)
                arrived(1, ("dline", k), deltas.at[k, 0])
                if of in far:
                    pl.when(z == 0)(functools.partial(spread_both, of))
                spread(k)

            if turn_k == 0:
                pass_early(0)
        sent[1] -= (len(others) + len(far) * plane) * 2
        for k in stops:
            if k > 0:
                pass_early(k)
            weigh(k)
        weight_squares()
        for k in stops:
            arrived(1, ("dplane", k), deltas.at[k, rest])
            hand_on = functools.partial(remote, 1, 0, ("delta", k), deltas.at[k], deltas.at[k], partner)
            if k in far:
                pl.when(z > 0)(hand_on)
            else:
                hand_on()
            for p in range(plane):
                update_sums(k, p)
        all_left(1)

    ratio = 0.2 * jnp.sqrt(wsq_ref[...] / (squares(usums) + 1e-06))
    row_ratio = masks[0] * ratio[0:1]
    for k in range(1, tensors):
        row_ratio = row_ratio + masks[k] * ratio[k:k + 1]
    ratios[...] = row_ratio


def finish(
    line, plane,
    weights, updates, ratios, m1_new, m2_new, mine, kept,
    weights_out, master_out, moment1_out, moment2_out,
    rounded, master_new, sem,
):
    me = lax.axis_index("dp")
    copies = [
        pltpu.make_async_copy(m1_new, moment1_out, sem.at[0]),
        pltpu.make_async_copy(m2_new, moment2_out, sem.at[1]),
    ]
    for copy in copies:
        copy.start()
    master_new[...] = kept[...] - ratios[pl.ds(me, 1), :] * mine[...]
    copies.append(pltpu.make_async_copy(master_new, master_out, sem.at[2]))
    copies[-1].start()

    def layer_copy(j):
        return pltpu.make_async_copy(rounded.at[j], weights_out.at[j], sem.at[3 + j])

    @pl.loop(0, line)
    def _(j):
        for at in range(plane):
            for side in range(2):
                scale = ratios[pl.ds((j * plane + at) * 2 + side, 1), :]
                new_row = weights[j, at, side] - scale * updates[j, at, side]
                rounded[j, at, side] = new_row.astype(jnp.bfloat16)
        layer_copy(j).start()

    for j in range(line):
        copies.append(layer_copy(j))
    for copy in copies:
        copy.wait()


def pinned(array):
    return pltpu.with_memory_space_constraint(array, pltpu.HBM)


def body(grads, master, moment1, moment2, tensor_rows, step_count):
    count = lax.axis_size("dp")
    line, plane = levels(count)
    row = (master.shape[0] // (8 * LANES), 8, LANES)
    f32, bf16 = jnp.float32, jnp.bfloat16
    hbm = pl.BlockSpec(memory_space=pltpu.HBM)
    vmem = pl.BlockSpec(memory_space=pltpu.VMEM)
    pair = (2,) + row
    table = (line, plane) + pair
    kept = jax.ShapeDtypeStruct(row, f32)
    leaving = 12 * line * plane
    state = pl.pallas_call(
        functools.partial(kernel, count, line, plane),
        out_shape=(
            jax.ShapeDtypeStruct(table, f32),
            jax.ShapeDtypeStruct(table, f32),
            jax.ShapeDtypeStruct((count, LANES), f32),
            kept, kept, kept, kept,
        ),
        in_specs=[hbm] * 5 + [pl.BlockSpec(memory_space=pltpu.SMEM)],
        out_specs=(vmem,) * 7,
        scratch_shapes=[
            pltpu.VMEM((line, plane, 2, 3) + row, bf16),
            pltpu.VMEM(table, bf16),
            pltpu.VMEM((leaving,) + row, bf16),
            pltpu.VMEM(table, f32),
            pltpu.VMEM(table, bf16),
            pltpu.VMEM(table, bf16),
            pltpu.VMEM((line, plane - 1) + pair, bf16),
            pltpu.VMEM((line, plane - 1) + pair, bf16),
            pltpu.VMEM((line - 1,) + pair, bf16),
            pltpu.VMEM((line - 1,) + pair, bf16),
            pltpu.VMEM((2, 3) + row, f32),
            pltpu.VMEM(pair, f32),
            pltpu.VMEM((count, LANES), f32),
            pltpu.VMEM((count, LANES), f32),
            pltpu.VMEM((tensor_rows.shape[0], count, LANES), f32),
            pltpu.VMEM((tensor_rows.shape[0], LANES), f32),
            pltpu.SMEM(tensor_rows.shape, jnp.int32),
            pltpu.SemaphoreType.DMA((4 * line + 5,)),
            pltpu.SemaphoreType.REGULAR,
            pltpu.SemaphoreType.REGULAR((line - 1,)),
            pltpu.SemaphoreType.REGULAR,
        ],
        compiler_params=pltpu.CompilerParams(
            collective_id=0, has_side_effects=True, vmem_limit_bytes=min(60, 20 + count // 4) * 1024 * 1024
        ),
        name="exchange",
    )(
        pinned(grads.reshape(table)),
        pinned(master.reshape(row)), pinned(moment1.reshape(row)), pinned(moment2.reshape(row)),
        pinned(tensor_rows), step_count,
    )
    outs = pl.pallas_call(
        functools.partial(finish, line, plane),
        out_shape=(jax.ShapeDtypeStruct(table, bf16), kept, kept, kept),
        in_specs=[vmem] * 7,
        out_specs=(hbm,) * 4,
        scratch_shapes=[
            pltpu.VMEM(table, bf16),
            pltpu.VMEM(row, f32),
            pltpu.SemaphoreType.DMA((3 + line,)),
        ],
        compiler_params=pltpu.CompilerParams(vmem_limit_bytes=24 * 1024 * 1024),
        name="finish",
    )(*state)
    return tuple(out.reshape(-1) for out in outs)


def solution(mesh):
    placed = (P("dp", None), P("dp"), P("dp"), P("dp"), P(), P())
    return jax.shard_map(
        body,
        mesh=mesh,
        in_specs=placed,
        out_specs=(P(), P("dp"), P("dp"), P("dp")),
        check_vma=False,
    )
```

```python
import functools
import math

import jax
import jax.numpy as jnp
import numpy as np
from jax import lax
from jax.experimental import pallas as pl
from jax.experimental.pallas import tpu as pltpu
from jax.sharding import PartitionSpec as P

LANES = 128
BETA1, BETA2 = 0.9, 0.999
STEP_BITS = 8


def levels(count):
    chips = count // 2
    bits = chips.bit_length() - 1
    plane = 1 << ((bits + 1) // 2)
    return chips // plane, plane


def flipped(value, mask):
    bit = 1
    while bit <= mask:
        if mask & bit:
            value = value + bit * (1 - 2 * (value // bit % 2))
        bit *= 2
    return value


def power(base, step):
    result = jnp.ones(step.shape, jnp.float32)
    for bit in range(STEP_BITS):
        factor = float(np.float32(float(np.float32(base)) ** (2**bit)))
        result = result * jnp.where((step // 2**bit) % 2 == 1, factor, 1.0)
    return result


def kernel(
    count, line, plane,
    grads, master, moment1, moment2, rows_in, step_ref,
    weights, updates, ratios, m1_new, m2_new, mine, kept,
    early, deltas, leaving, own, pair_send, pair_recv, plane_send, plane_recv,
    line_send, line_recv, state, grad_ref, wsums, usums, masks, wsq_ref, rows_ref,
    sems, plane_ready, line_ready, turn,
):
    me = lax.axis_index("dp")
    core = me % 2
    xy = me // 2 % plane
    z = me // (2 * plane)
    partner = me + 1 - 2 * core
    far_first = list(range(line - 1, 0, -1))
    near_first = far_first[::-1]
    others = list(range(plane - 1, 0, -1))
    order = sorted(near_first, key=lambda k: (bin(k).count("1"), -k))
    layers = order + [0]
    stops = [0] + near_first
    far = [line - 1]
    f32, bf16 = jnp.float32, jnp.bfloat16
    tensors = rows_ref.shape[0]

    def plane_peer(mask):
        return (z * plane + flipped(xy, mask)) * 2 + core

    def line_peer(mask):
        return (flipped(z, mask) * plane + xy) * 2 + core

    def signal(semaphore, peer):
        pl.semaphore_signal(semaphore, inc=1, device_id=(peer,), device_id_type=pl.DeviceIdType.MESH)

    barrier = pltpu.get_barrier_semaphore()
    signal(barrier, partner)
    for p in others:
        pl.when((core == 1) & (flipped(xy, p) > xy))(functools.partial(signal, barrier, plane_peer(p)))
    for k in far_first:
        pl.when(flipped(z, k) > z)(functools.partial(signal, barrier, line_peer(k)))

    def local(source, target, slot):
        copy = pltpu.make_async_copy(source, target, sems.at[slot])
        copy.start()
        return copy

    loads = {k: local(grads.at[flipped(z, k)], own.at[k], k) for k in layers}
    for i, part in enumerate((moment1, moment2, master)):
        local(part, state.at[core, i], 4 * line + 2)
    rows_load = local(rows_in, rows_ref, 4 * line + 3)

    def greet():
        pl.semaphore_wait(barrier, 1 + z + core * xy)
        for p in others:
            pl.when((core == 1) & (flipped(xy, p) < xy))(functools.partial(signal, plane_ready, plane_peer(p)))
        for k in far_first:
            pl.when(flipped(z, k) < z)(functools.partial(signal, line_ready.at[z - 1], line_peer(k)))

    step = jnp.full((8, LANES), step_ref[0], jnp.int32)
    first_scale = 1.0 - power(BETA1, step)
    second_scale = 1.0 - power(BETA2, step)

    def update_of(first, second, weight):
        return (first / first_scale) / (jnp.sqrt(second / second_scale) + 1e-06) + 0.1 * weight

    def make_row():
        ref = state.at[core]
        pltpu.make_async_copy(ref, ref, sems.at[4 * line + 2]).wait()
        weight = state[core, 2]
        kept[...] = weight
        high = weight.astype(bf16)
        early[0, 0, core, 0] = high
        early[0, 0, core, 1] = (weight - high.astype(f32)).astype(bf16)
        early[0, 0, core, 2] = update_of(0.9 * state[core, 0], 0.999 * state[core, 1], weight).astype(bf16)

    pools = {
        0: {"row": 2 * line, "grad": 3 * line, "delta": 0, "early": line, "line": 2 * line},
        1: {"row": 4 * line + 1, "state": 4 * line + 1, "line": 4 * line, "pair": line, "plane": 2 * line,
            "dplane": 0, "dline": line, "early": 3 * line},
    }
    sent = [0, 0]

    def remote(side, to, key, source, target, peer):
        name, k = key if isinstance(key, tuple) else (key, 0)
        pltpu.make_async_remote_copy(
            src_ref=source, dst_ref=target,
            send_sem=sems.at[4 * line + 4], recv_sem=sems.at[pools[to][name] + k],
            device_id=(peer,), device_id_type=pl.DeviceIdType.MESH,
        ).start()
        words = 2 if source.dtype == f32 else 1
        sent[side] += words * math.prod(source.shape[:-3])

    def wait_for(semaphore, ref):
        pltpu.make_async_copy(ref, ref, semaphore).wait()

    def arrived(side, key, ref):
        name, k = key if isinstance(key, tuple) else (key, 0)
        wait_for(sems.at[pools[side][name] + k], ref)

    def all_left(side):
        wait_for(sems.at[4 * line + 4], leaving.at[pl.ds(0, sent[side])])

    def place(k, p):
        return flipped(z, k), flipped(xy, p)

    def put_sums(sums, k, p, values):
        at = (flipped(z, k) * plane + flipped(xy, p)) * 2
        for side in range(2):
            total = jnp.sum(values[side] * values[side], axis=0)
            sums[pl.ds(at + side, 1), :] = jnp.sum(total, axis=0, keepdims=True)

    def tensor_masks():
        rows_load.wait()
        index = lax.broadcasted_iota(jnp.int32, (count, LANES), 0)
        start = jnp.int32(0)
        for k in range(tensors):
            end = start + rows_ref[k]
            masks[k] = ((index >= start) & (index < end)).astype(f32)
            start = end

    def squares(sums):
        values = sums[...]
        parts = [jnp.sum(masks[k] * values, axis=0, keepdims=True) for k in range(tensors)]
        return jnp.sum(jnp.concatenate(parts, axis=0), axis=1, keepdims=True)

    def weight_squares():
        wsq_ref[...] = jnp.broadcast_to(squares(wsums), wsq_ref.shape)

    def weight_sums(k, p):
        weight = early[k, p, :, 0].astype(f32) + early[k, p, :, 1].astype(f32)
        weights[place(k, p)] = weight
        put_sums(wsums, k, p, weight)

    def update_sums(k, p):
        update = early[k, p, :, 2].astype(f32) + deltas[k, p].astype(f32)
        updates[place(k, p)] = update
        put_sums(usums, k, p, update)

    rest = pl.ds(1, plane - 1)
    later = pl.ds(1, line - 1)

    @pl.when(core == 0)
    def _():
        greet()
        make_row()
        row = early.at[0, 0, 0]
        remote(0, 1, "row", row, row, partner)
        for k in layers:
            loads[k].wait()
            pair_send[k] = own[k].astype(bf16)
            remote(0, 1, ("pair", k), pair_send.at[k], pair_recv.at[k], partner)
        remote(0, 1, "state", state.at[0], state.at[0], partner)
        tensor_masks()
        arrived(0, "row", early.at[0, 0, 1])

        def spread(k):
            for p in others:
                remote(0, 1, ("early", k), early.at[k, 0], early.at[k, p], plane_peer(p) + 1)

        for to in range(line):
            @pl.when(z != to)
            def _():
                if to > 0:
                    pl.when(z < to)(functools.partial(pl.semaphore_wait, line_ready.at[to - 1], 1))
                k = jnp.bitwise_xor(z, to)
                remote(0, 0, ("line", k), early.at[0, 0], early.at[k, 0], (to * plane + xy) * 2)

        sent[0] -= math.prod(early.shape[2:4])

        pl.semaphore_wait(turn, 1)
        spread(0)
        weight_sums(0, 0)
        last = (z == line - 1).astype(jnp.int32)
        for i in range(line):
            of = i + last * (line - 2 - 2 * i)

            @pl.when((of != z) & (of >= 0))
            def _():
                k = jnp.bitwise_xor(z, of)
                arrived(0, ("line", k), early.at[k, 0])
                spread(k)
                remote(0, 1, ("early", k), early.at[k, 0], early.at[k, 0], partner)

        sent[0] -= plane * math.prod(early.shape[2:4])
        for k in near_first:
            weight_sums(k, 0)

        arrived(0, "grad", grad_ref.at[0])
        grad = grad_ref[0]
        new_m1 = 0.9 * state[0, 0] + 0.1 * grad
        new_m2 = 0.999 * state[0, 1] + 0.001 * grad * grad
        mine[...] = update_of(new_m1, new_m2, state[0, 2])
        m1_new[...] = new_m1
        m2_new[...] = new_m2
        for k in stops:
            arrived(0, ("early", k), early.at[k, rest])
            for p in range(1, plane):
                weight_sums(k, p)
        weight_squares()
        for k in stops:
            arrived(0, ("delta", k), deltas.at[k])
            for p in range(plane):
                update_sums(k, p)
        all_left(0)

    @pl.when(core == 1)
    def _():
        greet()
        make_row()
        row = early.at[0, 0, 1]
        remote(1, 0, "row", row, row, partner)
        for turn_k, k in enumerate(layers):
            loads[k].wait()
            if turn_k == 0:
                pl.when(xy < plane - 1)(functools.partial(pl.semaphore_wait, plane_ready, plane - 1 - xy))
            arrived(1, ("pair", k), pair_recv.at[k])
            for p in others:
                at = flipped(xy, p)
                plane_send[k, p - 1] = (own[k, at] + pair_recv[k, at].astype(f32)).astype(bf16)
                remote(1, 1, ("plane", k), plane_send.at[k, p - 1], plane_recv.at[k, p - 1], plane_peer(p))

        tensor_masks()
        all_left(1)
        sent[1] = 0
        signal(turn, partner)

        def pass_early(k):
            arrived(1, ("early", k), early.at[k] if k > 0 else early.at[k, rest])
            remote(1, 0, ("early", k), early.at[k, rest], early.at[k, rest], partner)

        def weigh(k):
            for p in range(plane):
                if (k, p) != (0, 0):
                    weight_sums(k, p)

        def plane_sum(k):
            arrived(1, ("plane", k), plane_recv.at[k])
            total = own[k, xy] + pair_recv[k, xy].astype(f32)
            for p in others:
                total = total + plane_recv[k, p - 1].astype(f32)
            return total

        for to in range(1, line):
            pl.when(z < to)(functools.partial(pl.semaphore_wait, line_ready.at[to - 1], 1))
        for k in order:
            line_send[k - 1] = plane_sum(k).astype(bf16)
            remote(1, 1, "line", line_send.at[k - 1], line_recv.at[k - 1], line_peer(k))
        grad = plane_sum(0)
        arrived(1, "row", early.at[0, pl.ds(0, 3), 0])
        arrived(1, "line", line_recv)
        for k in far_first:
            grad = grad + line_recv[k - 1].astype(f32)
        grad = grad / jnp.float32(count)
        new_m1 = 0.9 * state[:, 0] + 0.1 * grad
        new_m2 = 0.999 * state[:, 1] + 0.001 * grad * grad
        update = update_of(new_m1, new_m2, state[:, 2])
        deltas[0, 0] = (update - early[0, 0, :, 2].astype(f32)).astype(bf16)
        for k in far_first:
            remote(1, 1, ("dline", k), deltas.at[0, 0], deltas.at[k, 0], line_peer(k))

        def spread(k):
            for p in others:
                remote(1, 1, ("dplane", k), deltas.at[k, 0], deltas.at[k, p], plane_peer(p))

        def spread_both(k):
            for p in others:
                remote(1, 0, ("delta", k), deltas.at[k, 0], deltas.at[k, p], plane_peer(p) - 1)
            remote(1, 0, ("delta", k), deltas.at[k, 0], deltas.at[k, 0], partner)

        spread(0)
        grad_ref[...] = grad
        remote(1, 0, "grad", grad_ref.at[0], grad_ref.at[0], partner)
        mine[...] = update[1]
        m1_new[...] = new_m1[1]
        m2_new[...] = new_m2[1]
        weight_sums(0, 0)
        for turn_k, of in enumerate(near_first + [0]):
            @pl.when(z != of)
            def _():
                k = jnp.bitwise_xor(z, of)
                arrived(1, ("dline", k), deltas.at[k, 0])
                if of in far:
                    pl.when(z == 0)(functools.partial(spread_both, of))
                spread(k)

            if turn_k == 0:
                pass_early(0)
        sent[1] -= (len(others) + len(far) * plane) * 2
        for k in stops:
            if k > 0:
                pass_early(k)
            weigh(k)
        weight_squares()
        for k in stops:
            arrived(1, ("dplane", k), deltas.at[k, rest])
            hand_on = functools.partial(remote, 1, 0, ("delta", k), deltas.at[k], deltas.at[k], partner)
            if k in far:
                pl.when(z > 0)(hand_on)
            else:
                hand_on()
            for p in range(plane):
                update_sums(k, p)
        all_left(1)

    ratio = 0.2 * jnp.sqrt(wsq_ref[...] / (squares(usums) + 1e-06))
    row_ratio = masks[0] * ratio[0:1]
    for k in range(1, tensors):
        row_ratio = row_ratio + masks[k] * ratio[k:k + 1]
    ratios[...] = row_ratio


def finish(
    line, plane,
    weights, updates, ratios, m1_new, m2_new, mine, kept,
    weights_out, master_out, moment1_out, moment2_out,
    rounded, master_new, sem,
):
    me = lax.axis_index("dp")
    copies = [
        pltpu.make_async_copy(m1_new, moment1_out, sem.at[0]),
        pltpu.make_async_copy(m2_new, moment2_out, sem.at[1]),
    ]
    for copy in copies:
        copy.start()
    master_new[...] = kept[...] - ratios[pl.ds(me, 1), :] * mine[...]
    copies.append(pltpu.make_async_copy(master_new, master_out, sem.at[2]))
    copies[-1].start()

    def layer_copy(j):
        return pltpu.make_async_copy(rounded.at[j], weights_out.at[j], sem.at[3 + j])

    @pl.loop(0, line)
    def _(j):
        for at in range(plane):
            for side in range(2):
                scale = ratios[pl.ds((j * plane + at) * 2 + side, 1), :]
                new_row = weights[j, at, side] - scale * updates[j, at, side]
                rounded[j, at, side] = new_row.astype(jnp.bfloat16)
        layer_copy(j).start()

    for j in range(line):
        copies.append(layer_copy(j))
    for copy in copies:
        copy.wait()


def pinned(array):
    return pltpu.with_memory_space_constraint(array, pltpu.HBM)


def body(grads, master, moment1, moment2, tensor_rows, step_count):
    count = lax.axis_size("dp")
    line, plane = levels(count)
    row = (master.shape[0] // (8 * LANES), 8, LANES)
    f32, bf16 = jnp.float32, jnp.bfloat16
    hbm = pl.BlockSpec(memory_space=pltpu.HBM)
    vmem = pl.BlockSpec(memory_space=pltpu.VMEM)
    pair = (2,) + row
    table = (line, plane) + pair
    kept = jax.ShapeDtypeStruct(row, f32)
    leaving = 12 * line * plane
    state = pl.pallas_call(
        functools.partial(kernel, count, line, plane),
        out_shape=(
            jax.ShapeDtypeStruct(table, f32),
            jax.ShapeDtypeStruct(table, f32),
            jax.ShapeDtypeStruct((count, LANES), f32),
            kept, kept, kept, kept,
        ),
        in_specs=[hbm] * 5 + [pl.BlockSpec(memory_space=pltpu.SMEM)],
        out_specs=(vmem,) * 7,
        scratch_shapes=[
            pltpu.VMEM((line, plane, 2, 3) + row, bf16),
            pltpu.VMEM(table, bf16),
            pltpu.VMEM((leaving,) + row, bf16),
            pltpu.VMEM(table, f32),
            pltpu.VMEM(table, bf16),
            pltpu.VMEM(table, bf16),
            pltpu.VMEM((line, plane - 1) + pair, bf16),
            pltpu.VMEM((line, plane - 1) + pair, bf16),
            pltpu.VMEM((line - 1,) + pair, bf16),
            pltpu.VMEM((line - 1,) + pair, bf16),
            pltpu.VMEM((2, 3) + row, f32),
            pltpu.VMEM(pair, f32),
            pltpu.VMEM((count, LANES), f32),
            pltpu.VMEM((count, LANES), f32),
            pltpu.VMEM((tensor_rows.shape[0], count, LANES), f32),
            pltpu.VMEM((tensor_rows.shape[0], LANES), f32),
            pltpu.SMEM(tensor_rows.shape, jnp.int32),
            pltpu.SemaphoreType.DMA((4 * line + 5,)),
            pltpu.SemaphoreType.REGULAR,
            pltpu.SemaphoreType.REGULAR((line - 1,)),
            pltpu.SemaphoreType.REGULAR,
        ],
        compiler_params=pltpu.CompilerParams(
            collective_id=0, has_side_effects=True, vmem_limit_bytes=min(60, 20 + count // 4) * 1024 * 1024
        ),
        name="exchange",
    )(
        pinned(grads.reshape(table)),
        pinned(master.reshape(row)), pinned(moment1.reshape(row)), pinned(moment2.reshape(row)),
        pinned(tensor_rows), step_count,
    )
    outs = pl.pallas_call(
        functools.partial(finish, line, plane),
        out_shape=(jax.ShapeDtypeStruct(table, bf16), kept, kept, kept),
        in_specs=[vmem] * 7,
        out_specs=(hbm,) * 4,
        scratch_shapes=[
            pltpu.VMEM(table, bf16),
            pltpu.VMEM(row, f32),
            pltpu.SemaphoreType.DMA((3 + line,)),
        ],
        compiler_params=pltpu.CompilerParams(vmem_limit_bytes=24 * 1024 * 1024),
        name="finish",
    )(*state)
    return tuple(out.reshape(-1) for out in outs)


def solution(mesh):
    placed = (P("dp", None), P("dp"), P("dp"), P("dp"), P(), P())
    return jax.shard_map(
        body,
        mesh=mesh,
        in_specs=placed,
        out_specs=(P(), P("dp"), P("dp"), P("dp")),
        check_vma=False,
    )
```

```python
import functools
import math

import jax
import jax.numpy as jnp
import numpy as np
from jax import lax
from jax.experimental import pallas as pl
from jax.experimental.pallas import tpu as pltpu
from jax.sharding import PartitionSpec as P

LANES = 128
BETA1, BETA2 = 0.9, 0.999
STEP_BITS = 8


def levels(count):
    chips = count // 2
    bits = chips.bit_length() - 1
    plane = 1 << ((bits + 1) // 2)
    return chips // plane, plane


def flipped(value, mask):
    bit = 1
    while bit <= mask:
        if mask & bit:
            value = value + bit * (1 - 2 * (value // bit % 2))
        bit *= 2
    return value


def power(base, step):
    result = jnp.ones(step.shape, jnp.float32)
    for bit in range(STEP_BITS):
        factor = float(np.float32(float(np.float32(base)) ** (2**bit)))
        result = result * jnp.where((step // 2**bit) % 2 == 1, factor, 1.0)
    return result


def kernel(
    count, line, plane,
    grads, master, moment1, moment2, rows_in, step_ref,
    weights, updates, ratios, m1_new, m2_new, mine, kept,
    early, deltas, leaving, own, pair_send, pair_recv, plane_send, plane_recv,
    line_send, line_recv, state, grad_ref, wsums, usums, masks, wsq_ref, rows_ref,
    sems, plane_ready, line_ready, turn,
):
    me = lax.axis_index("dp")
    core = me % 2
    xy = me // 2 % plane
    z = me // (2 * plane)
    partner = me + 1 - 2 * core
    far_first = list(range(line - 1, 0, -1))
    near_first = far_first[::-1]
    others = list(range(plane - 1, 0, -1))
    order = sorted(near_first, key=lambda k: (bin(k).count("1"), -k))
    layers = order + [0]
    stops = [0] + near_first
    far = [line - 1]
    f32, bf16 = jnp.float32, jnp.bfloat16
    tensors = rows_ref.shape[0]

    def plane_peer(mask):
        return (z * plane + flipped(xy, mask)) * 2 + core

    def line_peer(mask):
        return (flipped(z, mask) * plane + xy) * 2 + core

    def signal(semaphore, peer):
        pl.semaphore_signal(semaphore, inc=1, device_id=(peer,), device_id_type=pl.DeviceIdType.MESH)

    barrier = pltpu.get_barrier_semaphore()
    signal(barrier, partner)
    for p in others:
        pl.when((core == 1) & (flipped(xy, p) > xy))(functools.partial(signal, barrier, plane_peer(p)))
    for k in far_first:
        pl.when(flipped(z, k) > z)(functools.partial(signal, barrier, line_peer(k)))

    def local(source, target, slot):
        copy = pltpu.make_async_copy(source, target, sems.at[slot])
        copy.start()
        return copy

    loads = {k: local(grads.at[flipped(z, k)], own.at[k], k) for k in layers}
    for i, part in enumerate((moment1, moment2, master)):
        local(part, state.at[core, i], 4 * line + 2)
    rows_load = local(rows_in, rows_ref, 4 * line + 3)

    def greet():
        pl.semaphore_wait(barrier, 1 + z + core * xy)
        for p in others:
            pl.when((core == 1) & (flipped(xy, p) < xy))(functools.partial(signal, plane_ready, plane_peer(p)))
        for k in far_first:
            pl.when(flipped(z, k) < z)(functools.partial(signal, line_ready.at[z - 1], line_peer(k)))

    step = jnp.full((8, LANES), step_ref[0], jnp.int32)
    first_scale = 1.0 - power(BETA1, step)
    second_scale = 1.0 - power(BETA2, step)

    def update_of(first, second, weight):
        return (first / first_scale) / (jnp.sqrt(second / second_scale) + 1e-06) + 0.1 * weight

    def make_row():
        ref = state.at[core]
        pltpu.make_async_copy(ref, ref, sems.at[4 * line + 2]).wait()
        weight = state[core, 2]
        kept[...] = weight
        high = weight.astype(bf16)
        early[0, 0, core, 0] = high
        early[0, 0, core, 1] = (weight - high.astype(f32)).astype(bf16)
        early[0, 0, core, 2] = update_of(0.9 * state[core, 0], 0.999 * state[core, 1], weight).astype(bf16)

    pools = {
        0: {"row": 2 * line, "grad": 3 * line, "delta": 0, "early": line, "line": 2 * line},
        1: {"row": 4 * line + 1, "state": 4 * line + 1, "line": 4 * line, "pair": line, "plane": 2 * line,
            "dplane": 0, "dline": line, "early": 3 * line},
    }
    sent = [0, 0]

    def remote(side, to, key, source, target, peer):
        name, k = key if isinstance(key, tuple) else (key, 0)
        pltpu.make_async_remote_copy(
            src_ref=source, dst_ref=target,
            send_sem=sems.at[4 * line + 4], recv_sem=sems.at[pools[to][name] + k],
            device_id=(peer,), device_id_type=pl.DeviceIdType.MESH,
        ).start()
        words = 2 if source.dtype == f32 else 1
        sent[side] += words * math.prod(source.shape[:-3])

    def wait_for(semaphore, ref):
        pltpu.make_async_copy(ref, ref, semaphore).wait()

    def arrived(side, key, ref):
        name, k = key if isinstance(key, tuple) else (key, 0)
        wait_for(sems.at[pools[side][name] + k], ref)

    def all_left(side):
        wait_for(sems.at[4 * line + 4], leaving.at[pl.ds(0, sent[side])])

    def place(k, p):
        return flipped(z, k), flipped(xy, p)

    def put_sums(sums, k, p, values):
        at = (flipped(z, k) * plane + flipped(xy, p)) * 2
        for side in range(2):
            total = jnp.sum(values[side] * values[side], axis=0)
            sums[pl.ds(at + side, 1), :] = jnp.sum(total, axis=0, keepdims=True)

    def tensor_masks():
        rows_load.wait()
        index = lax.broadcasted_iota(jnp.int32, (count, LANES), 0)
        start = jnp.int32(0)
        for k in range(tensors):
            end = start + rows_ref[k]
            masks[k] = ((index >= start) & (index < end)).astype(f32)
            start = end

    def squares(sums):
        values = sums[...]
        parts = [jnp.sum(masks[k] * values, axis=0, keepdims=True) for k in range(tensors)]
        return jnp.sum(jnp.concatenate(parts, axis=0), axis=1, keepdims=True)

    def weight_squares():
        wsq_ref[...] = jnp.broadcast_to(squares(wsums), wsq_ref.shape)

    def weight_sums(k, p):
        weight = early[k, p, :, 0].astype(f32) + early[k, p, :, 1].astype(f32)
        weights[place(k, p)] = weight
        put_sums(wsums, k, p, weight)

    def update_sums(k, p):
        update = early[k, p, :, 2].astype(f32) + deltas[k, p].astype(f32)
        updates[place(k, p)] = update
        put_sums(usums, k, p, update)

    rest = pl.ds(1, plane - 1)
    later = pl.ds(1, line - 1)

    @pl.when(core == 0)
    def _():
        greet()
        make_row()
        row = early.at[0, 0, 0]
        remote(0, 1, "row", row, row, partner)
        for k in layers:
            loads[k].wait()
            pair_send[k] = own[k].astype(bf16)
            remote(0, 1, ("pair", k), pair_send.at[k], pair_recv.at[k], partner)
        remote(0, 1, "state", state.at[0], state.at[0], partner)
        tensor_masks()
        arrived(0, "row", early.at[0, 0, 1])

        def spread(k):
            for p in others:
                remote(0, 1, ("early", k), early.at[k, 0], early.at[k, p], plane_peer(p) + 1)

        for to in range(line):
            @pl.when(z != to)
            def _():
                if to > 0:
                    pl.when(z < to)(functools.partial(pl.semaphore_wait, line_ready.at[to - 1], 1))
                k = jnp.bitwise_xor(z, to)
                remote(0, 0, ("line", k), early.at[0, 0], early.at[k, 0], (to * plane + xy) * 2)

        sent[0] -= math.prod(early.shape[2:4])

        pl.semaphore_wait(turn, 1)
        spread(0)
        weight_sums(0, 0)
        last = (z == line - 1).astype(jnp.int32)
        for i in range(line):
            of = i + last * (line - 2 - 2 * i)

            @pl.when((of != z) & (of >= 0))
            def _():
                k = jnp.bitwise_xor(z, of)
                arrived(0, ("line", k), early.at[k, 0])
                spread(k)
                remote(0, 1, ("early", k), early.at[k, 0], early.at[k, 0], partner)

        sent[0] -= plane * math.prod(early.shape[2:4])
        for k in near_first:
            weight_sums(k, 0)

        arrived(0, "grad", grad_ref.at[0])
        grad = grad_ref[0]
        new_m1 = 0.9 * state[0, 0] + 0.1 * grad
        new_m2 = 0.999 * state[0, 1] + 0.001 * grad * grad
        mine[...] = update_of(new_m1, new_m2, state[0, 2])
        m1_new[...] = new_m1
        m2_new[...] = new_m2
        for k in stops:
            arrived(0, ("early", k), early.at[k, rest])
            for p in range(1, plane):
                weight_sums(k, p)
        weight_squares()
        for k in stops:
            arrived(0, ("delta", k), deltas.at[k])
            for p in range(plane):
                update_sums(k, p)
        all_left(0)

    @pl.when(core == 1)
    def _():
        greet()
        make_row()
        row = early.at[0, 0, 1]
        remote(1, 0, "row", row, row, partner)
        for turn_k, k in enumerate(layers):
            loads[k].wait()
            if turn_k == 0:
                pl.when(xy < plane - 1)(functools.partial(pl.semaphore_wait, plane_ready, plane - 1 - xy))
            arrived(1, ("pair", k), pair_recv.at[k])
            for p in others:
                at = flipped(xy, p)
                plane_send[k, p - 1] = (own[k, at] + pair_recv[k, at].astype(f32)).astype(bf16)
                remote(1, 1, ("plane", k), plane_send.at[k, p - 1], plane_recv.at[k, p - 1], plane_peer(p))

        tensor_masks()
        all_left(1)
        sent[1] = 0
        signal(turn, partner)

        def pass_early(k):
            arrived(1, ("early", k), early.at[k] if k > 0 else early.at[k, rest])
            remote(1, 0, ("early", k), early.at[k, rest], early.at[k, rest], partner)

        def weigh(k):
            for p in range(plane):
                if (k, p) != (0, 0):
                    weight_sums(k, p)

        def plane_sum(k):
            arrived(1, ("plane", k), plane_recv.at[k])
            total = own[k, xy] + pair_recv[k, xy].astype(f32)
            for p in others:
                total = total + plane_recv[k, p - 1].astype(f32)
            return total

        for to in range(1, line):
            pl.when(z < to)(functools.partial(pl.semaphore_wait, line_ready.at[to - 1], 1))
        for k in order:
            line_send[k - 1] = plane_sum(k).astype(bf16)
            remote(1, 1, "line", line_send.at[k - 1], line_recv.at[k - 1], line_peer(k))
        grad = plane_sum(0)
        arrived(1, "row", early.at[0, pl.ds(0, 3), 0])
        arrived(1, "line", line_recv)
        for k in far_first:
            grad = grad + line_recv[k - 1].astype(f32)
        grad = grad / jnp.float32(count)
        new_m1 = 0.9 * state[:, 0] + 0.1 * grad
        new_m2 = 0.999 * state[:, 1] + 0.001 * grad * grad
        update = update_of(new_m1, new_m2, state[:, 2])
        deltas[0, 0] = (update - early[0, 0, :, 2].astype(f32)).astype(bf16)
        for k in far_first:
            remote(1, 1, ("dline", k), deltas.at[0, 0], deltas.at[k, 0], line_peer(k))

        def spread(k):
            for p in others:
                remote(1, 1, ("dplane", k), deltas.at[k, 0], deltas.at[k, p], plane_peer(p))

        def spread_both(k):
            for p in others:
                remote(1, 0, ("delta", k), deltas.at[k, 0], deltas.at[k, p], plane_peer(p) - 1)
            remote(1, 0, ("delta", k), deltas.at[k, 0], deltas.at[k, 0], partner)

        spread(0)
        grad_ref[...] = grad
        remote(1, 0, "grad", grad_ref.at[0], grad_ref.at[0], partner)
        mine[...] = update[1]
        m1_new[...] = new_m1[1]
        m2_new[...] = new_m2[1]
        weight_sums(0, 0)
        for turn_k, of in enumerate(near_first + [0]):
            @pl.when(z != of)
            def _():
                k = jnp.bitwise_xor(z, of)
                arrived(1, ("dline", k), deltas.at[k, 0])
                if of in far:
                    pl.when(z == 0)(functools.partial(spread_both, of))
                spread(k)

            if turn_k == 0:
                pass_early(0)
        sent[1] -= (len(others) + len(far) * plane) * 2
        for k in stops:
            if k > 0:
                pass_early(k)
            weigh(k)
        weight_squares()
        for k in stops:
            arrived(1, ("dplane", k), deltas.at[k, rest])
            hand_on = functools.partial(remote, 1, 0, ("delta", k), deltas.at[k], deltas.at[k], partner)
            if k in far:
                pl.when(z > 0)(hand_on)
            else:
                hand_on()
            for p in range(plane):
                update_sums(k, p)
        all_left(1)

    ratio = 0.2 * jnp.sqrt(wsq_ref[...] / (squares(usums) + 1e-06))
    row_ratio = masks[0] * ratio[0:1]
    for k in range(1, tensors):
        row_ratio = row_ratio + masks[k] * ratio[k:k + 1]
    ratios[...] = row_ratio


def finish(
    line, plane,
    weights, updates, ratios, m1_new, m2_new, mine, kept,
    weights_out, master_out, moment1_out, moment2_out,
    rounded, master_new, sem,
):
    me = lax.axis_index("dp")
    copies = [
        pltpu.make_async_copy(m1_new, moment1_out, sem.at[0]),
        pltpu.make_async_copy(m2_new, moment2_out, sem.at[1]),
    ]
    for copy in copies:
        copy.start()
    master_new[...] = kept[...] - ratios[pl.ds(me, 1), :] * mine[...]
    copies.append(pltpu.make_async_copy(master_new, master_out, sem.at[2]))
    copies[-1].start()

    def layer_copy(j):
        return pltpu.make_async_copy(rounded.at[j], weights_out.at[j], sem.at[3 + j])

    for j in range(line):
        for at in range(plane):
            for side in range(2):
                scale = ratios[pl.ds((j * plane + at) * 2 + side, 1), :]
                new_row = weights[j, at, side] - scale * updates[j, at, side]
                rounded[j, at, side] = new_row.astype(jnp.bfloat16)
        layer_copy(j).start()

    for j in range(line):
        copies.append(layer_copy(j))
    for copy in copies:
        copy.wait()


def pinned(array):
    return pltpu.with_memory_space_constraint(array, pltpu.HBM)


def body(grads, master, moment1, moment2, tensor_rows, step_count):
    count = lax.axis_size("dp")
    line, plane = levels(count)
    row = (master.shape[0] // (8 * LANES), 8, LANES)
    f32, bf16 = jnp.float32, jnp.bfloat16
    hbm = pl.BlockSpec(memory_space=pltpu.HBM)
    vmem = pl.BlockSpec(memory_space=pltpu.VMEM)
    pair = (2,) + row
    table = (line, plane) + pair
    kept = jax.ShapeDtypeStruct(row, f32)
    leaving = 12 * line * plane
    state = pl.pallas_call(
        functools.partial(kernel, count, line, plane),
        out_shape=(
            jax.ShapeDtypeStruct(table, f32),
            jax.ShapeDtypeStruct(table, f32),
            jax.ShapeDtypeStruct((count, LANES), f32),
            kept, kept, kept, kept,
        ),
        in_specs=[hbm] * 5 + [pl.BlockSpec(memory_space=pltpu.SMEM)],
        out_specs=(vmem,) * 7,
        scratch_shapes=[
            pltpu.VMEM((line, plane, 2, 3) + row, bf16),
            pltpu.VMEM(table, bf16),
            pltpu.VMEM((leaving,) + row, bf16),
            pltpu.VMEM(table, f32),
            pltpu.VMEM(table, bf16),
            pltpu.VMEM(table, bf16),
            pltpu.VMEM((line, plane - 1) + pair, bf16),
            pltpu.VMEM((line, plane - 1) + pair, bf16),
            pltpu.VMEM((line - 1,) + pair, bf16),
            pltpu.VMEM((line - 1,) + pair, bf16),
            pltpu.VMEM((2, 3) + row, f32),
            pltpu.VMEM(pair, f32),
            pltpu.VMEM((count, LANES), f32),
            pltpu.VMEM((count, LANES), f32),
            pltpu.VMEM((tensor_rows.shape[0], count, LANES), f32),
            pltpu.VMEM((tensor_rows.shape[0], LANES), f32),
            pltpu.SMEM(tensor_rows.shape, jnp.int32),
            pltpu.SemaphoreType.DMA((4 * line + 5,)),
            pltpu.SemaphoreType.REGULAR,
            pltpu.SemaphoreType.REGULAR((line - 1,)),
            pltpu.SemaphoreType.REGULAR,
        ],
        compiler_params=pltpu.CompilerParams(
            collective_id=0, has_side_effects=True, vmem_limit_bytes=min(60, 20 + count // 4) * 1024 * 1024
        ),
        name="exchange",
    )(
        pinned(grads.reshape(table)),
        pinned(master.reshape(row)), pinned(moment1.reshape(row)), pinned(moment2.reshape(row)),
        pinned(tensor_rows), step_count,
    )
    outs = pl.pallas_call(
        functools.partial(finish, line, plane),
        out_shape=(jax.ShapeDtypeStruct(table, bf16), kept, kept, kept),
        in_specs=[vmem] * 7,
        out_specs=(hbm,) * 4,
        scratch_shapes=[
            pltpu.VMEM(table, bf16),
            pltpu.VMEM(row, f32),
            pltpu.SemaphoreType.DMA((3 + line,)),
        ],
        compiler_params=pltpu.CompilerParams(vmem_limit_bytes=24 * 1024 * 1024),
        name="finish",
    )(*state)
    return tuple(out.reshape(-1) for out in outs)


def solution(mesh):
    placed = (P("dp", None), P("dp"), P("dp"), P("dp"), P(), P())
    return jax.shard_map(
        body,
        mesh=mesh,
        in_specs=placed,
        out_specs=(P(), P("dp"), P("dp"), P("dp")),
        check_vma=False,
    )
```
